32 devices in a mesh: row: 8 (over z, core), col: 4 (over y, x).
Axes of the slice: x: 2, y: 2, z: 4, core: 2. Of those that a mesh axis runs over, the one named last changes fastest.
Arguments:
- ancestor_inverse: float32 [12288, 12288], P('row', 'col'), may hold values from -6 to 6
- panel: float32 [5632, 512], P('col', 'row'), may hold values from -0.078125 to 0.078125
- unit_inverse: float32 [512, 512], P('row'), may hold values from -1 to 1, as said below
- pivot_inverse: float32 [512, 512], P('row', 'col'), may hold values from -6 to 6
- panel_blocks: int32 [44], replicated, may hold values from 0 to 95, as said below
Outputs:
- inverse_row: float32 [512, 12288], P('col', 'row')
- diagonal_block: float32 [512, 512], P('row', 'col')
The draws below stay inside these ranges and needn't reach their ends.
Inputs may be any that keep to these rules, and one draw needn't show every extreme that they name: `panel_blocks`: Distinct, in no particular order. Among the window blocks c * 24 to c * 24 + 23 of any process column c at most 12 are listed, and exactly 12 for some columns. `unit_inverse`: unit lower triangular: ones on the diagonal, zeros above it.
All inputs are finite; a program needn't handle non-finite values.
Results may differ from the reference program's by a relative error of at most 0.00011.
Values sent between devices are 32-bit elements; how exact they have to be, the bound alone decides.
A program may use at most 128 MiB of HBM per device.

```python
import jax
import jax.numpy as jnp
from jax import lax

W = 512
BLK = 128
NWB = 96
R = 12288
PB = 44
P_SIZE = 5632
N_COL = 4


def draw_panel_blocks(key, part):
    range_blocks = NWB // N_COL
    slot_count = range_blocks // 2
    column_order = jax.random.permutation(jax.random.fold_in(key, 11), N_COL)
    counts_used = jnp.where(column_order % 2 == 0, slot_count, slot_count - 2)
    base_ranks = jnp.tile(jnp.arange(range_blocks, dtype=jnp.int32)[None, :], (N_COL, 1))
    ranks = jax.random.permutation(jax.random.fold_in(key, 12), base_ranks, axis=1, independent=True)
    chosen = ranks < counts_used[:, None]
    first_local = jnp.argmax(chosen.astype(jnp.int32), axis=1).astype(jnp.int32)
    firsts = jnp.arange(N_COL, dtype=jnp.int32) * range_blocks + first_local
    local_ids = jnp.arange(range_blocks, dtype=jnp.int32)[None, :]
    rest_mask = (chosen & (local_ids != first_local[:, None])).reshape(-1).astype(jnp.int32)
    per_shard = PB // N_COL
    rest_ids = jnp.argsort(1 - rest_mask, stable=True)[:PB - N_COL].astype(jnp.int32)
    rest_part = rest_ids.reshape(N_COL, per_shard - 1)
    leading = jnp.roll(firsts, -(N_COL // 2))
    stored = jnp.concatenate([leading[:, None], rest_part], axis=1).reshape(-1)
    return stored.astype(jnp.int32)


def draw_unit_inverse(key, part):
    spread = 0.5 / W ** 0.5
    entries = jax.random.truncated_normal(jax.random.fold_in(key, 21), -4.0, 4.0, (W, W), jnp.float32) * spread
    row_ids = jnp.arange(W, dtype=jnp.int32)[:, None]
    col_ids = jnp.arange(W, dtype=jnp.int32)[None, :]
    below = jnp.where(row_ids > col_ids, entries, 0.0)
    return (below + jnp.where(row_ids == col_ids, 1.0, 0.0)).astype(jnp.float32)


def block_scale(stream_key, extent, shards, low, high):
    factor_of, own = 1.0, jax.random.fold_in(stream_key, 6)
    for axis_at, shards_of in shards:
        steps = jnp.exp(jax.random.uniform(jax.random.fold_in(own, axis_at), (shards_of,), jnp.float32, low / len(shards), high / len(shards)))
        factor_of = factor_of * jnp.repeat(steps, extent[axis_at] // shards_of).reshape([-1 if axis == axis_at else 1 for axis in range(len(extent))])
    return factor_of


def bell_draw(rng, dims, width, bound, split=(), kind=jnp.bfloat16):
    drawn = width * jax.random.normal(rng, dims, jnp.float32)
    if split:
        drawn = drawn * block_scale(rng, dims, split, -0.22, 0.18)
    return jnp.clip(drawn, -bound, bound).astype(kind)


def setup_inputs(seed: int = 0) -> dict:
    streams_of = jax.random.split(jax.random.key(seed), 6)
    return {
        "ancestor_inverse": bell_draw(streams_of[0], (R, R), 1.0, 6.0, ((0, 8), (1, 4)), jnp.float32),
        "panel": bell_draw(streams_of[1], (P_SIZE, W), P_SIZE ** -0.5, 0.078125, ((0, 4), (1, 8)), jnp.float32),
        "unit_inverse": draw_unit_inverse(jax.random.fold_in(streams_of[5], 71), 0),
        "pivot_inverse": bell_draw(streams_of[3], (W, W), 1.0, 6.0, ((0, 8), (1, 4)), jnp.float32),
        "panel_blocks": draw_panel_blocks(jax.random.fold_in(streams_of[5], 71), 0),
    }


def reference(ancestor_inverse, panel, unit_inverse, pivot_inverse, panel_blocks):
    highest = lax.Precision.HIGHEST
    normal = jnp.dot(panel, unit_inverse, precision=highest, preferred_element_type=jnp.float32)
    blocked = ancestor_inverse.reshape(R, NWB, BLK)
    columns = jnp.take(blocked, panel_blocks, axis=1).reshape(R, PB * BLK)
    column_inverse = -jnp.dot(columns, normal, precision=highest, preferred_element_type=jnp.float32)
    listed = jnp.take(column_inverse.reshape(NWB, BLK, W), panel_blocks, axis=0).reshape(PB * BLK, W)
    product = jnp.dot(normal.T, listed, precision=highest, preferred_element_type=jnp.float32)
    diagonal_block = pivot_inverse - product
    return column_inverse.T, diagonal_block
```

```python
import functools

import jax
import jax.numpy as jnp
from jax import lax
from jax.experimental import pallas as pl
from jax.experimental.pallas import tpu as pltpu
from jax.sharding import PartitionSpec as P

BLK = 128
NT = (((1,), (1,)), ((), ()))


def select_kernel(per_shard, slots, ids_ref, live_ref, gathered_ref, out_ref):
    for slot in range(slots):
        block = ids_ref[slot]
        start = pl.multiple_of((block % per_shard) * BLK, BLK)
        value = gathered_ref[block // per_shard, :, pl.ds(start, BLK)]
        out_ref[:, slot * BLK : (slot + 1) * BLK] = jnp.where(live_ref[slot] > 0, value, 0.0)


def select(gathered, ids, live):
    slots = ids.shape[0]
    per_shard = gathered.shape[2] // BLK
    smem = pl.BlockSpec(memory_space=pltpu.SMEM)
    vmem = pl.BlockSpec(memory_space=pltpu.VMEM)
    return pl.pallas_call(
        functools.partial(select_kernel, per_shard, slots),
        out_shape=jax.ShapeDtypeStruct((gathered.shape[1], slots * BLK), jnp.float32),
        in_specs=[smem, smem, vmem],
        out_specs=vmem,
    )(ids, live, gathered)


def place_kernel(ids_ref, live_ref, value_ref, out_ref):
    out_ref[...] = jnp.where(live_ref[pl.program_id(0)] > 0, value_ref[...], 0.0)


def place(value, ids, live):
    width, blocks = value.shape[0], ids.shape[0]
    return pl.pallas_call(
        place_kernel,
        out_shape=jax.ShapeDtypeStruct((width, blocks * BLK), jnp.float32),
        grid_spec=pltpu.PrefetchScalarGridSpec(
            num_scalar_prefetch=2,
            grid=(blocks,),
            in_specs=[pl.BlockSpec((width, BLK), lambda b, ids, live: (0, ids[b]))],
            out_specs=pl.BlockSpec((width, BLK), lambda b, ids, live: (0, b)),
        ),
    )(ids, live, value)


def halves(value):
    high = value.astype(jnp.bfloat16)
    return high, (value - high.astype(jnp.float32)).astype(jnp.bfloat16)


def product_kernel(group, ids_ref, normal_ref, *refs):
    out_ref = refs[group]

    @pl.when(pl.program_id(1) == 0)
    def _():
        out_ref[...] = jnp.zeros_like(out_ref)

    n_high, n_low = halves(normal_ref[...])
    if group == 1:
        block = refs[0][...]
    else:
        block = jnp.concatenate([ref[...] for ref in refs[:group]], axis=1)
    a_high, a_low = halves(block)
    dot = functools.partial(
        lax.dot_general, dimension_numbers=NT, preferred_element_type=jnp.float32
    )
    out_ref[...] -= dot(n_high, a_high) + (dot(n_high, a_low) + dot(n_low, a_high))


def product(normal, ancestor, ids):
    width, slots = normal.shape[0], ids.shape[0]
    rows = ancestor.shape[0]
    group = 2 if slots % 2 == 0 else 1
    tile = 512 if rows % 512 == 0 else BLK

    def column(k):
        return pl.BlockSpec((tile, BLK), lambda i, j, ids: (i, ids[j * group + k]))

    return pl.pallas_call(
        functools.partial(product_kernel, group),
        out_shape=jax.ShapeDtypeStruct((width, rows), jnp.float32),
        grid_spec=pltpu.PrefetchScalarGridSpec(
            num_scalar_prefetch=1,
            grid=(rows // tile, slots // group),
            in_specs=[pl.BlockSpec((width, group * BLK), lambda i, j, ids: (0, j))]
            + [column(k) for k in range(group)],
            out_specs=pl.BlockSpec((width, tile), lambda i, j, ids: (0, i)),
        ),
        compiler_params=pltpu.CompilerParams(
            dimension_semantics=("arbitrary", "arbitrary"), vmem_limit_bytes=32 << 20
        ),
        cost_estimate=pl.CostEstimate(
            flops=6 * width * rows * slots * BLK,
            bytes_accessed=4 * (rows * slots * BLK + 2 * width * rows),
            transcendentals=0,
        ),
    )(ids, normal, *([ancestor] * group))


def on_device(ancestor_inverse, panel, unit_inverse, pivot_inverse, panel_blocks):
    high = lax.Precision.HIGH
    row_index = lax.axis_index("row")
    col_index = lax.axis_index("col")
    rows_here, cols_here = ancestor_inverse.shape
    width = unit_inverse.shape[1]
    block_total = panel_blocks.shape[0]
    range_blocks = cols_here // BLK
    row_blocks = rows_here // BLK
    first_block = col_index * range_blocks
    slot_count = range_blocks // 2

    gathered = lax.all_gather(panel.T, "col", axis=0, tiled=False)
    half = width // 2
    unit = [
        lax.all_gather(unit_inverse[:, k * half : (k + 1) * half], "row", axis=0, tiled=True)
        for k in range(2)
    ]

    in_range = (panel_blocks >= first_block) & (panel_blocks < first_block + range_blocks)
    order = jnp.arange(block_total, dtype=jnp.int32)
    upto = order[None, :] <= order[:, None]
    rank_of = jnp.sum((upto & in_range[None, :]).astype(jnp.int32), axis=1) - 1
    slot_ids = jnp.arange(slot_count, dtype=jnp.int32)
    selected = in_range[None, :] & (rank_of[None, :] == slot_ids[:, None])
    stored_ids = jnp.sum(jnp.where(selected, order[None, :], 0), axis=1)
    chosen_ids = jnp.sum(jnp.where(selected, panel_blocks[None, :], 0), axis=1)
    slot_live = jnp.sum(selected.astype(jnp.int32), axis=1)
    window_ids = jnp.where(slot_live > 0, chosen_ids, -1)
    local_ids = jnp.clip(chosen_ids - first_block, 0, range_blocks - 1)
    row_ids = row_index * row_blocks + jnp.arange(row_blocks, dtype=jnp.int32)
    match = window_ids[None, :] == row_ids[:, None]
    row_slot = jnp.sum(jnp.where(match, slot_ids[None, :], 0), axis=1)
    row_live = jnp.sum(match.astype(jnp.int32), axis=1)

    chosen = select(gathered, stored_ids, slot_live)
    window = lax.all_gather(chosen, "row", axis=0, tiled=True)
    normal = jnp.concatenate(
        [
            lax.dot_general(
                part,
                window,
                (((0,), (0,)), ((), ())),
                precision=high,
                preferred_element_type=jnp.float32,
            )
            for part in unit
        ],
        axis=0,
    )
    own_window = lax.psum(place(normal, row_slot, row_live), "col")
    inverse_tile = lax.psum_scatter(
        product(normal, ancestor_inverse, local_ids), "col", scatter_dimension=0, tiled=True
    )
    crossed = -lax.dot_general(
        own_window, inverse_tile, NT, precision=high, preferred_element_type=jnp.float32
    )
    parts = lax.all_to_all(
        crossed.reshape(width // pivot_inverse.shape[0], *pivot_inverse.shape), "row", 0, 0
    )
    diagonal_block = pivot_inverse + jnp.sum(parts, axis=0)
    return (inverse_tile, diagonal_block)


def solution(mesh):
    return jax.shard_map(
        on_device,
        mesh=mesh,
        in_specs=(P("row", "col"), P("col", "row"), P("row", None), P("row", "col"), P()),
        out_specs=(P("col", "row"), P("row", "col")),
        check_vma=False,
    )
```

```python
import functools

import jax
import jax.numpy as jnp
from jax import lax
from jax.experimental import pallas as pl
from jax.experimental.pallas import tpu as pltpu
from jax.sharding import PartitionSpec as P

BLK = 128
NT = (((1,), (1,)), ((), ()))


def select_kernel(per_shard, ids_ref, live_ref, gathered_ref, out_ref):
    slots = out_ref.shape[2] // BLK
    for target in range(out_ref.shape[0]):
        for slot in range(slots):
            at = target * slots + slot
            block = ids_ref[at]
            start = pl.multiple_of((block % per_shard) * BLK, BLK)
            value = gathered_ref[block // per_shard, :, pl.ds(start, BLK)]
            out_ref[target, :, slot * BLK : (slot + 1) * BLK] = jnp.where(
                live_ref[at] > 0, value, 0.0
            )


def select(gathered, ids, live, targets):
    slots = ids.shape[0] // targets
    per_shard = gathered.shape[2] // BLK
    smem = pl.BlockSpec(memory_space=pltpu.SMEM)
    vmem = pl.BlockSpec(memory_space=pltpu.VMEM)
    return pl.pallas_call(
        functools.partial(select_kernel, per_shard),
        out_shape=jax.ShapeDtypeStruct((targets, gathered.shape[1], slots * BLK), jnp.float32),
        in_specs=[smem, smem, vmem],
        out_specs=vmem,
    )(ids, live, gathered)


def halves(value):
    high = value.astype(jnp.bfloat16)
    return high, (value - high.astype(jnp.float32)).astype(jnp.bfloat16)


def product_kernel(group, ids_ref, normal_ref, *refs):
    out_ref = refs[group]

    @pl.when(pl.program_id(1) == 0)
    def _():
        out_ref[...] = jnp.zeros_like(out_ref)

    n_high, n_low = halves(normal_ref[...])
    if group == 1:
        block = refs[0][...]
    else:
        block = jnp.concatenate([ref[...] for ref in refs[:group]], axis=1)
    a_high, a_low = halves(block)
    dot = functools.partial(
        lax.dot_general, dimension_numbers=NT, preferred_element_type=jnp.float32
    )
    out_ref[...] -= dot(n_high, a_high) + (dot(n_high, a_low) + dot(n_low, a_high))


def product(normal, ancestor, ids):
    width, slots = normal.shape[0], ids.shape[0]
    rows = ancestor.shape[0]
    group = 2 if slots % 2 == 0 else 1
    tile = 512 if rows % 512 == 0 else BLK

    def column(k):
        return pl.BlockSpec((tile, BLK), lambda i, j, ids: (i, ids[j * group + k]))

    return pl.pallas_call(
        functools.partial(product_kernel, group),
        out_shape=jax.ShapeDtypeStruct((width, rows), jnp.float32),
        grid_spec=pltpu.PrefetchScalarGridSpec(
            num_scalar_prefetch=1,
            grid=(rows // tile, slots // group),
            in_specs=[pl.BlockSpec((width, group * BLK), lambda i, j, ids: (0, j))]
            + [column(k) for k in range(group)],
            out_specs=pl.BlockSpec((width, tile), lambda i, j, ids: (0, i)),
        ),
        compiler_params=pltpu.CompilerParams(
            dimension_semantics=("arbitrary", "arbitrary"), vmem_limit_bytes=32 << 20
        ),
        cost_estimate=pl.CostEstimate(
            flops=6 * width * rows * slots * BLK,
            bytes_accessed=4 * (rows * slots * BLK + 2 * width * rows),
            transcendentals=0,
        ),
    )(ids, normal, *([ancestor] * group))


def on_device(ancestor_inverse, panel, unit_inverse, pivot_inverse, panel_blocks):
    high = lax.Precision.HIGH
    col_index = lax.axis_index("col")
    rows_here, cols_here = ancestor_inverse.shape
    width = unit_inverse.shape[1]
    block_total = panel_blocks.shape[0]
    range_blocks = cols_here // BLK
    row_blocks = rows_here // BLK
    first_block = col_index * range_blocks
    slot_count = range_blocks // 2

    gathered = lax.all_gather(panel.T, "col", axis=0, tiled=False)
    half = width // 2
    unit = [
        lax.all_gather(unit_inverse[:, k * half : (k + 1) * half], "row", axis=0, tiled=True)
        for k in range(2)
    ]

    in_range = (panel_blocks >= first_block) & (panel_blocks < first_block + range_blocks)
    order = jnp.arange(block_total, dtype=jnp.int32)
    upto = order[None, :] <= order[:, None]
    rank_of = jnp.sum((upto & in_range[None, :]).astype(jnp.int32), axis=1) - 1
    slot_ids = jnp.arange(slot_count, dtype=jnp.int32)
    selected = in_range[None, :] & (rank_of[None, :] == slot_ids[:, None])
    stored_ids = jnp.sum(jnp.where(selected, order[None, :], 0), axis=1)
    chosen_ids = jnp.sum(jnp.where(selected, panel_blocks[None, :], 0), axis=1)
    slot_live = jnp.sum(selected.astype(jnp.int32), axis=1)
    local_ids = jnp.clip(chosen_ids - first_block, 0, range_blocks - 1)
    gathered, unit = lax.optimization_barrier((gathered, unit))
    unit = jnp.concatenate(unit, axis=1)
    rows, cols = lax.axis_size("row"), lax.axis_size("col")
    chosen = select(gathered, stored_ids, slot_live, 1)[0]
    window = lax.all_gather(chosen, "row", axis=0, tiled=True)

    match = panel_blocks[None, :] == jnp.arange(rows * row_blocks, dtype=jnp.int32)[:, None]
    block_ids = jnp.sum(jnp.where(match, order[None, :], 0), axis=1)
    block_live = jnp.sum(match.astype(jnp.int32), axis=1)
    part = panel.shape[1] // cols
    share = lax.dynamic_slice_in_dim(gathered, col_index * part, part, 1)
    listed = lax.all_to_all(select(share, block_ids, block_live, rows), "row", 0, 0)
    listed = lax.all_gather(listed, "col", axis=0, tiled=False).reshape(width, rows_here)
    unit_mixed = unit.reshape(rows, cols, part, width).transpose(1, 0, 2, 3).reshape(width, width)

    def normalise(factor, value):
        return lax.dot_general(
            factor,
            value,
            (((0,), (0,)), ((), ())),
            precision=high,
            preferred_element_type=jnp.float32,
        )

    normal = normalise(unit, window)
    own_window = normalise(unit_mixed, listed)
    inverse_tile = lax.psum_scatter(
        product(normal, ancestor_inverse, local_ids), "col", scatter_dimension=0, tiled=True
    )
    crossed = -lax.dot_general(
        own_window, inverse_tile, NT, precision=high, preferred_element_type=jnp.float32
    )
    parts = lax.all_to_all(
        crossed.reshape(width // pivot_inverse.shape[0], *pivot_inverse.shape), "row", 0, 0
    )
    diagonal_block = pivot_inverse + jnp.sum(parts, axis=0)
    return (inverse_tile, diagonal_block)


def solution(mesh):
    return jax.shard_map(
        on_device,
        mesh=mesh,
        in_specs=(P("row", "col"), P("col", "row"), P("row", None), P("row", "col"), P()),
        out_specs=(P("col", "row"), P("row", "col")),
        check_vma=False,
    )
```
